32 devices in a mesh: section: 16 (over z, x, core), tp: 2 (over y).
Axes of the slice: x: 2, y: 2, z: 4, core: 2. Of those that a mesh axis runs over, the one named last changes fastest.
Arguments:
- carried: bfloat16 [16, 256, 5120], P('section', 'tp'), may hold values from -6 to 6
- carried_segments: int32 [16, 256], P('section'), may hold values from 0 to 31, as said below
- fresh_batch: bfloat16 [2, 256, 5120], P(None, 'tp'), may hold values from -6 to 6
- fresh_segments: int32 [2, 256], replicated, may hold values from 0 to 31, as said below
- qkv_weight: bfloat16 [16, 5120, 3, 2048], P('section', None, None, 'tp'), may hold values from -3.354102 to 3.354102
- out_weight: bfloat16 [16, 2048, 5120], P('section', 'tp'), may hold values from -0.09375 to 0.09375
- norm_gain: bfloat16 [16, 2560], P('section'), may hold values from 0.099609375 to 1.8984375
Outputs:
- layer_outputs: bfloat16 [2, 16, 256, 5120], P(None, 'section', 'tp')
- shadow_outputs: bfloat16 [16, 256, 5120], P('section', 'tp')
The draws below stay inside these ranges and needn't reach their ends.
Inputs may be any that keep to these rules, and one draw needn't show every extreme that they name: `carried_segments`: document ids of each micro-batch's 512 tokens, read in token order across its two halves, start at 0, never fall, and rise by one at each document start; every micro-batch holds exactly 32 documents. `fresh_segments`: the same law for the entering micro-batch.
All inputs are finite; a program needn't handle non-finite values.
Results may differ from the reference program's by a relative error of at most 0.019.
Values may be sent and summed in bfloat16 or wider, within the bound.
A program may use at most 128 MiB of HBM per device.

```python
import jax
import jax.numpy as jnp
from jax import lax

D = 5120
HEADS = 32
HD = 128
TOK = 512
STEPS = 2
SECTIONS = 8
HALF = 256
N_TP = 2


def segment_ids(key, count):
    pieces = max(2, TOK // 16)
    keys = jax.random.split(key, count)
    orders = jax.vmap(lambda single: jax.random.permutation(single, TOK - 1))(keys)
    chosen = orders[:, :pieces - 1] + 1
    marks = jnp.zeros((count, TOK), jnp.int32)
    marks = marks.at[jnp.arange(count)[:, None], chosen].set(1)
    marks = marks.at[:, 0].set(1)
    return (jnp.cumsum(marks, axis=1) - 1).astype(jnp.int32)


def draw_carried_segments(key, part):
    return segment_ids(jax.random.fold_in(key, 21), SECTIONS).reshape(SECTIONS * 2, TOK // 2)


def draw_fresh_segments(key, part):
    return segment_ids(jax.random.fold_in(key, 22), 1).reshape(2, TOK // 2)


def draw_qkv_weight(key, part):
    columns = HEADS * HD // 2
    drawn = jax.random.truncated_normal(jax.random.fold_in(key, 11), -6.0, 6.0, (SECTIONS * 2, D, 3, columns), jnp.float32) * D ** (-0.5)
    return drawn.astype(jnp.bfloat16)


def levels(own_key, extent, cuts, smallest, high):
    loudness = 1.0
    for position, blocks in cuts:
        steps = jax.random.uniform(jax.random.fold_in(jax.random.fold_in(own_key, 6), position), (blocks,), jnp.float32, smallest / len(cuts), high / len(cuts))
        loudness = loudness * jnp.repeat(jnp.exp(steps), extent[position] // blocks).reshape((-1,) + (1,) * (len(extent) - 1 - position))
    return loudness


def normal_values(own_key, dims, spread, reach, cuts=(), held_as=jnp.bfloat16):
    level = levels(own_key, dims, cuts, -0.22, 0.18) if cuts else 1.0
    values = jax.random.normal(own_key, dims, jnp.float32) * spread * level
    return jnp.minimum(jnp.maximum(values, -reach), reach).astype(held_as)


def setup_inputs(seed: int = 0) -> dict:
    arg_keys = jax.random.split(jax.random.key(seed), 8)
    carried = normal_values(arg_keys[0], (2 * SECTIONS, HALF, D), 1.0, 6.0, ((0, 16), (1, 2)))
    carried_segments = draw_carried_segments(jax.random.fold_in(arg_keys[7], 71), 0)
    fresh_batch = normal_values(arg_keys[2], (2, HALF, D), 1.0, 6.0, ((1, 2),))
    fresh_segments = draw_fresh_segments(jax.random.fold_in(arg_keys[7], 71), 0)
    qkv_weight = draw_qkv_weight(jax.random.fold_in(arg_keys[7], 71), 0)
    out_weight = normal_values(arg_keys[5], (2 * SECTIONS, HEADS * HD // 2, D), (HEADS * HD) ** -0.5, 0.09375, ((0, 16), (1, 2)))
    norm_gain = jnp.clip(1.0 + 0.18 * jax.random.normal(arg_keys[6], (2 * SECTIONS, D // 2), jnp.float32), 0.099609375, 1.8984375).astype(jnp.bfloat16)
    return dict(carried=carried, carried_segments=carried_segments, fresh_batch=fresh_batch, fresh_segments=fresh_segments, qkv_weight=qkv_weight, out_weight=out_weight, norm_gain=norm_gain)


eps = 1e-05
rope_base = 10000.0

def normalize(values, gain):
    widened = values.astype(jnp.float32)
    power = lax.optimization_barrier(jnp.mean(widened * widened, axis=-1, keepdims=True))
    return (widened * lax.rsqrt(power + eps) * gain.astype(jnp.float32)).astype(jnp.bfloat16)

def rotate(values, positions):
    half_dim = values.shape[-1] // 2
    frequency = rope_base ** (-(jnp.arange(half_dim, dtype=jnp.float32) * 2.0 / values.shape[-1]))
    angles = positions.astype(jnp.float32)[:, None] * frequency[None, :]
    cosine = jnp.cos(angles)[:, None, :]
    sine = jnp.sin(angles)[:, None, :]
    leading = values[..., :half_dim]
    trailing = values[..., half_dim:]
    return jnp.concatenate([leading * cosine - trailing * sine, trailing * cosine + leading * sine], axis=-1)

def attend(projected, positions, segments):
    count = projected.shape[0]
    width = projected.shape[1] // 3
    parts = projected.reshape(count, 3, width // HD, HD)
    queries = rotate(parts[:, 0], positions).astype(jnp.bfloat16)
    keyed = rotate(parts[:, 1], positions).astype(jnp.bfloat16)
    values = parts[:, 2].astype(jnp.bfloat16)
    scores = jnp.einsum('qhd,khd->hqk', queries.astype(jnp.float32), keyed.astype(jnp.float32)) * HD ** (-0.5)
    visible = (positions[None, :] <= positions[:, None]) & (segments[None, :] == segments[:, None])
    masked = jnp.where(visible[None], scores, -1e+30)
    highest = lax.optimization_barrier(jnp.max(masked, axis=-1, keepdims=True))
    weights = jnp.where(visible[None], jnp.exp(masked - highest), 0.0)
    shares = (weights / lax.optimization_barrier(jnp.sum(weights, axis=-1, keepdims=True))).astype(jnp.bfloat16)
    mixed = jnp.einsum('hqk,khd->qhd', shares.astype(jnp.float32), values.astype(jnp.float32))
    return mixed.astype(jnp.bfloat16).reshape(count, width)

def layer(bundle):
    rows, segments, gain, weights_in, weights_out = bundle
    matrix = jnp.transpose(weights_in, (1, 2, 0, 3)).reshape(D, 3 * HEADS * HD)
    normed = normalize(rows, gain)
    projected = jnp.dot(normed, matrix, preferred_element_type=jnp.float32)
    positions = jnp.arange(TOK, dtype=jnp.int32)
    mixed = attend(projected, positions, segments)
    groups = 2 * N_TP
    width = HEADS * HD // groups
    blocks = mixed.reshape(TOK, groups, width).astype(jnp.float32)
    out_blocks = weights_out.reshape(groups, width, D).astype(jnp.float32)
    partials = jnp.einsum('tgc,gcd->gtd', blocks, out_blocks)
    rounded = lax.optimization_barrier(partials.astype(jnp.bfloat16)).astype(jnp.float32)
    return (rows.astype(jnp.float32) + lax.optimization_barrier(jnp.sum(rounded, axis=0))).astype(jnp.bfloat16)

def reference(carried, carried_segments, fresh_batch, fresh_segments, qkv_weight, out_weight, norm_gain):
    inputs_one = carried.reshape(SECTIONS, TOK, D)
    segments_one = carried_segments.reshape(SECTIONS, TOK)
    gains = norm_gain.reshape(SECTIONS, D)
    weights_in = qkv_weight.reshape(SECTIONS, 2, D, 3, HEADS * HD // 2)
    weights_out = out_weight.reshape(SECTIONS, HEADS * HD, D)
    outputs_one = lax.map(layer, (inputs_one, segments_one, gains, weights_in, weights_out))
    inputs_two = jnp.concatenate([fresh_batch.reshape(1, TOK, D), outputs_one[:-1]], axis=0)
    segments_two = jnp.concatenate([fresh_segments.reshape(1, TOK), segments_one[:-1]], axis=0)
    outputs_two = lax.map(layer, (inputs_two, segments_two, gains, weights_in, weights_out))
    shadow = jnp.concatenate([outputs_two[1:], jnp.zeros((1, TOK, D), jnp.bfloat16)], axis=0)
    stacked = jnp.stack([outputs_one, outputs_two]).reshape(STEPS, 2 * SECTIONS, HALF, D)
    return (stacked, shadow.reshape(2 * SECTIONS, HALF, D))
```

```python
import functools

import jax
import jax.numpy as jnp
from jax import lax
from jax.experimental import pallas as pl
from jax.experimental.pallas import tpu as pltpu
from jax.sharding import PartitionSpec as P

HD = 128
CHUNKS = 4
JOINED = 2
QUERY_BLOCKS = 4
LANES = 128
PROJECT_WIDTH = 512
LOG2E = 1.4426950408889634

eps = 1e-05
rope_base = 10000.0


def from_core(value):
    pairs = [(i, i ^ 1) for i in range(lax.axis_size("section"))]
    return lax.ppermute(value, "section", pairs)


def from_ahead(value, by):
    count = lax.axis_size("tp")
    return lax.ppermute(value, "tp", [((i + by) % count, i) for i in range(count)])


def to_ahead(value, by):
    count = lax.axis_size("tp")
    return lax.ppermute(value, "tp", [(i, (i + by) % count) for i in range(count)])


def shifted(value, by):
    count = lax.axis_size("section")
    pairs = [(i, i + by) for i in range(count) if 0 <= i + by < count]
    return lax.ppermute(value, "section", pairs)


def attention_kernel(q_ref, k_ref, v_ref, cosine_ref, sine_ref, power_ref, bias_ref, out_ref, *, depth):
    power = jnp.sum(power_ref[...], axis=-1, keepdims=True) / depth
    scale = lax.rsqrt(power + eps)
    cosine = cosine_ref[...] * scale
    sine = sine_ref[...] * scale

    def rotated(values):
        return values * cosine + pltpu.roll(values, HD // 2, 1) * sine

    queries = (rotated(q_ref[...]) * (HD ** (-0.5) * LOG2E)).astype(jnp.bfloat16)
    keyed = rotated(k_ref[...]).astype(jnp.bfloat16)
    values = (v_ref[...] * scale).astype(jnp.bfloat16)
    rows = queries.shape[0] // QUERY_BLOCKS
    for block in range(QUERY_BLOCKS):
        part = slice(block * rows, (block + 1) * rows)
        scores = lax.dot_general(
            queries[part], keyed, (((1,), (1,)), ((), ())), preferred_element_type=jnp.float32
        ) + bias_ref[part, :]
        weights = jnp.exp2(scores - jnp.max(scores, axis=-1, keepdims=True))
        total = jnp.sum(weights, axis=-1, keepdims=True)
        mixed = jnp.dot(
            weights.astype(jnp.bfloat16), values, preferred_element_type=jnp.float32
        )
        out_ref[part, :] = (mixed / total).astype(jnp.bfloat16)


def attend(projected, cosine, sine, power, bias, depth):
    count, width = projected.shape[0], projected.shape[1] // 3
    number = width // HD
    heads = [pl.BlockSpec((count, HD), lambda h, i=i: (0, h + i * number)) for i in range(3)]
    return pl.pallas_call(
        functools.partial(attention_kernel, depth=depth),
        grid=(number,),
        out_shape=jax.ShapeDtypeStruct((count, width), jnp.bfloat16),
        in_specs=heads
        + [pl.BlockSpec(each.shape, lambda h: (0, 0)) for each in (cosine, sine, power, bias)],
        out_specs=heads[0],
        cost_estimate=pl.CostEstimate(
            flops=4 * count * count * width,
            bytes_accessed=14 * count * width,
            transcendentals=count * count * width // HD,
        ),
        name="attend",
    )(projected, projected, projected, cosine, sine, power, bias)


def project_kernel(count, *refs):
    pieces, (gain_ref, weights_ref) = refs[:count], refs[count : count + 2]
    earlier, (out_ref, power_ref, scaled) = refs[count + 2 : -3], refs[-3:]

    @pl.when(pl.program_id(0) == 0)
    def _():
        high, step = pieces[0].shape
        deep = scaled.shape[0] // high
        for i in range(deep):
            rows = slice(i * high, (i + 1) * high)
            power = earlier[1][rows, :] if earlier else 0.0
            for c in range(count // deep):
                cols = slice(c * step, (c + 1) * step)
                widened = pieces[c * deep + i][...].astype(jnp.float32)
                scaled[rows, cols] = (widened * gain_ref[:, cols]).astype(jnp.bfloat16)
                for lane in range(0, step, LANES):
                    power = power + widened[:, lane : lane + LANES] ** 2
            power_ref[rows, :] = power

    product = jnp.dot(scaled[...], weights_ref[0], preferred_element_type=jnp.float32)
    out_ref[...] = product + earlier[0][...] if earlier else product


def project(pieces, gain, weights_in, block, earlier):
    count = len(pieces)
    step = pieces[0].shape[1] * JOINED
    total = count // JOINED * pieces[0].shape[0]
    kinds, _, width = weights_in.shape
    across = width // PROJECT_WIDTH
    sums = pl.BlockSpec((total, PROJECT_WIDTH), lambda j: (0, j))
    squares = pl.BlockSpec((total, LANES), lambda j: (0, 0))
    return pl.pallas_call(
        functools.partial(project_kernel, count),
        grid=(kinds * across,),
        out_shape=(
            jax.ShapeDtypeStruct((total, kinds * width), jnp.float32),
            jax.ShapeDtypeStruct((total, LANES), jnp.float32),
        ),
        in_specs=[pl.BlockSpec(piece.shape, lambda j: (0, 0)) for piece in pieces]
        + [
            pl.BlockSpec((1, step), lambda j: (0, block)),
            pl.BlockSpec((1, step, PROJECT_WIDTH), lambda j: (j // across, block, j % across)),
        ]
        + [sums, squares][: len(earlier)],
        out_specs=(sums, squares),
        scratch_shapes=[pltpu.VMEM((total, step), jnp.bfloat16)],
        cost_estimate=pl.CostEstimate(
            flops=2 * total * step * kinds * width,
            bytes_accessed=2 * step * kinds * width + 8 * total * kinds * width,
            transcendentals=0,
        ),
        name="project",
    )(*pieces, gain, weights_in, *earlier)


def gather_and_project(own, weights_in, gain, groups):
    sums = ()
    for c in range(0, len(own), JOINED):
        pieces = []
        for mine in own[c : c + JOINED]:
            rest = [from_ahead(mine, k) for k in range(1, groups)]
            pieces += [mine, *rest, from_core(mine), *[from_core(r) for r in rest]]
        sums = project(pieces, gain, weights_in, c // JOINED, sums)
    return sums


def out_chunks(mixed, weights, own, groups):
    block, step = own[0].shape
    half = mixed.shape[0] // 2
    taken, outputs = [], []
    for c, mine in enumerate(own):
        if c >= 2:
            mixed, taken[c - 2] = lax.optimization_barrier((mixed, taken[c - 2]))
        columns = weights[:, c * step : (c + 1) * step]
        give = jnp.dot(mixed[half:], columns, preferred_element_type=jnp.float32)
        taken.append(from_core(give.astype(jnp.bfloat16)))
        outputs.append(jnp.dot(mixed[:half], columns, preferred_element_type=jnp.float32))
    for c, mine in enumerate(own):
        part = outputs[c] + taken[c].astype(jnp.float32)
        total = mine.astype(jnp.float32) + part[:block]
        for k in range(1, groups):
            sent = part[k * block : (k + 1) * block].astype(jnp.bfloat16)
            total = total + to_ahead(sent, k).astype(jnp.float32)
        outputs[c] = total.astype(jnp.bfloat16)
    return outputs


def per_device(
    carried, carried_segments, fresh_batch, fresh_segments, qkv_weight, out_weight, norm_gain
):
    groups = lax.axis_size("tp")
    placed = lax.axis_index("section")
    parity = placed % 2
    at_start = placed // 2 == 0
    own_one = carried[0]
    block, depth = own_one.shape
    half = block * groups
    weights_out = out_weight[0]
    weights_in = jnp.transpose(qkv_weight[0], (1, 0, 2))
    step = depth // CHUNKS

    first_row = lax.axis_index("tp") * block
    within = (jnp.arange(half, dtype=jnp.int32) + first_row) % half
    positions = jnp.concatenate([parity * half + within, (1 - parity) * half + within])

    def turned(ids):
        return lax.dynamic_slice(jnp.concatenate([ids, ids], -1), (0, first_row), (2, half)).reshape(-1)

    other_segments, other_gain = from_core((carried_segments[0], norm_gain[0]))
    ids_one = jnp.stack([carried_segments[0], other_segments])
    gain = jnp.where(
        parity == 0,
        jnp.concatenate([norm_gain[0], other_gain]),
        jnp.concatenate([other_gain, norm_gain[0]]),
    ).astype(jnp.float32)[None]
    fresh_ids = jnp.where(parity == 0, fresh_segments, fresh_segments[::-1])
    ids_two = jnp.where(at_start, fresh_ids, shifted(ids_one, 2))
    half_dim = HD // 2
    frequency = rope_base ** (-(jnp.arange(half_dim, dtype=jnp.float32) * 2.0 / HD))
    angles = positions.astype(jnp.float32)[:, None] * frequency[None, :]
    cosine, sine = jnp.cos(angles), jnp.sin(angles)
    cosine = jnp.concatenate([cosine, cosine], axis=-1)
    sine = jnp.concatenate([-sine, sine], axis=-1)
    causal = positions[None, :] <= positions[:, None]

    def bias(ids):
        ids = turned(ids)
        return jnp.where(causal & (ids[None, :] == ids[:, None]), 0.0, -1e30)

    def columns(rows):
        return [
            lax.optimization_barrier(rows[:, c * step : (c + 1) * step]) for c in range(CHUNKS)
        ]

    own_one = columns(own_one)
    entering = columns(lax.dynamic_index_in_dim(fresh_batch, parity, 0, keepdims=False))

    projected, power = gather_and_project(own_one, weights_in, gain, groups)
    mixed = attend(projected, cosine, sine, power, bias(ids_one), depth)
    first = out_chunks(mixed, weights_out, own_one, groups)
    own_two = [jnp.where(at_start, e, shifted(done, 2)) for e, done in zip(entering, first)]

    projected, power = gather_and_project(own_two, weights_in, gain, groups)
    mixed = attend(projected, cosine, sine, power, bias(ids_two), depth)
    second = out_chunks(mixed, weights_out, own_two, groups)
    shadow = [shifted(done, -2) for done in second]
    first, second, shadow = (jnp.concatenate(v, axis=-1) for v in (first, second, shadow))
    return (jnp.stack([first, second])[:, None], shadow[None])


def solution(mesh):
    return jax.shard_map(
        per_device,
        mesh=mesh,
        in_specs=(
            P("section", "tp", None),
            P("section", None),
            P(None, "tp", None),
            P(),
            P("section", None, None, "tp"),
            P("section", "tp", None),
            P("section", None),
        ),
        out_specs=(P(None, "section", "tp", None), P("section", "tp", None)),
        check_vma=False,
    )
```
